32 devices in a mesh: third: 4 (over z), second: 2 (over y), group: 4 (over x, core).
Axes of the slice: x: 2, y: 2, z: 4, core: 2. Of those that a mesh axis runs over, the one named last changes fastest.
Arguments:
- x_one: bfloat16 [65536, 768], P(('third', 'second', 'group'))
- z_one: bfloat16 [65536, 3072], P(('third', 'second', 'group'))
- x_two: bfloat16 [65536, 768], P(('third', 'second', 'group'))
- z_two: bfloat16 [65536, 3072], P(('third', 'second', 'group'))
- grad_out: bfloat16 [65536, 768], P(('third', 'second', 'group'))
- w1_in: bfloat16 [768, 3072], replicated
- w1_out: bfloat16 [3072, 768], replicated
- w2_in: bfloat16 [768, 3072], replicated
- w2_out: bfloat16 [3072, 768], replicated
Outputs:
- output 1: float32 [3072, 768], replicated
- output 2: float32 [768, 3072], replicated
- output 3: float32 [3072, 768], replicated
- output 4: float32 [768, 3072], replicated
- output 5: bfloat16 [65536, 768], P(('third', 'second', 'group'))
All inputs are finite; a program needn't handle non-finite values.
Results may differ from the reference program's by a relative error of at most 0.00509931.
Values are sent between devices in bfloat16 or wider.
A program may use at most 1 GiB of HBM per device.

```python
import math
import jax
import jax.numpy as jnp
from jax import lax

D = 768
FF = 3072
TOKENS = 2048
DEVICES = 32

INV_ROOT_TWO = math.sqrt(0.5)
INV_ROOT_TWO_PI = 1.0 / math.sqrt(2.0 * math.pi)


def gelu_pair(z_pre):
    z_val = z_pre.astype(jnp.float32)
    cdf_val = 0.5 * (1.0 + lax.erf(z_val * INV_ROOT_TWO))
    hidden = (z_val * cdf_val).astype(jnp.bfloat16)
    slope = cdf_val + z_val * jnp.exp(-0.5 * z_val * z_val) * INV_ROOT_TWO_PI
    return hidden, slope


def block_backward(x_in, z_pre, grad_y, w_in, w_out):
    hidden, slope = gelu_pair(z_pre)
    w_out_grad = jnp.dot(hidden.T, grad_y, preferred_element_type=jnp.float32).astype(jnp.bfloat16)
    grad_hidden = jnp.dot(grad_y, w_out.T, preferred_element_type=jnp.float32)
    grad_pre = (grad_hidden * slope).astype(jnp.bfloat16)
    w_in_grad = jnp.dot(x_in.T, grad_pre, preferred_element_type=jnp.float32).astype(jnp.bfloat16)
    grad_x = (grad_y.astype(jnp.float32) + jnp.dot(grad_pre, w_in.T, preferred_element_type=jnp.float32)).astype(jnp.bfloat16)
    return w_out_grad, w_in_grad, grad_x


def setup_inputs(seed: int = 0) -> dict:
    keys = jax.random.split(jax.random.key(seed), 9)
    row_count = DEVICES * TOKENS

    def normal_draw(key_part, shape_in, factor):
        return (jax.random.normal(key_part, shape_in, jnp.float32) * factor).astype(jnp.bfloat16)

    return dict(
        x_one=normal_draw(keys[0], (row_count, D), 1.0),
        z_one=normal_draw(keys[1], (row_count, FF), 1.0),
        x_two=normal_draw(keys[2], (row_count, D), 1.0),
        z_two=normal_draw(keys[3], (row_count, FF), 1.0),
        grad_out=normal_draw(keys[4], (row_count, D), row_count ** -0.25),
        w1_in=normal_draw(keys[5], (D, FF), D ** -0.5),
        w1_out=normal_draw(keys[6], (FF, D), FF ** -0.5),
        w2_in=normal_draw(keys[7], (D, FF), D ** -0.5),
        w2_out=normal_draw(keys[8], (FF, D), FF ** -0.5),
    )


def reference(x_one, z_one, x_two, z_two, grad_out, w1_in, w1_out, w2_in, w2_out):
    def by_device(arr):
        return arr.reshape(DEVICES, TOKENS, arr.shape[-1])

    def device_step(run_sums, batch):
        x_one_dev, z_one_dev, x_two_dev, z_two_dev, grad_dev = batch
        w2o_grad, w2i_grad, dx_two = block_backward(x_two_dev, z_two_dev, grad_dev, w2_in, w2_out)
        w1o_grad, w1i_grad, dx_one = block_backward(x_one_dev, z_one_dev, dx_two, w1_in, w1_out)
        new_sums = tuple(run_sum + grad_part.astype(jnp.float32) for run_sum, grad_part in zip(run_sums, (w2o_grad, w2i_grad, w1o_grad, w1i_grad)))
        return new_sums, dx_one

    zero_sums = (
        jnp.zeros((FF, D), jnp.float32),
        jnp.zeros((D, FF), jnp.float32),
        jnp.zeros((FF, D), jnp.float32),
        jnp.zeros((D, FF), jnp.float32),
    )
    batches = (by_device(x_one), by_device(z_one), by_device(x_two), by_device(z_two), by_device(grad_out))
    total_sums, grad_rows = lax.scan(device_step, zero_sums, batches)
    return (total_sums[0], total_sums[1], total_sums[2], total_sums[3], grad_rows.reshape(DEVICES * TOKENS, D))
```

```python
import math
import jax
import jax.numpy as jnp
from jax import lax
from jax.sharding import PartitionSpec as P

AXES = ('third', 'second', 'group')
INV_ROOT_TWO = math.sqrt(0.5)
INV_ROOT_TWO_PI = 1.0 / math.sqrt(2.0 * math.pi)
CONTRACT_ROWS = (((0,), (0,)), ((), ()))
CONTRACT_COLS = (((1,), (1,)), ((), ()))


def gelu_pair(z_pre):
    z_val = z_pre.astype(jnp.float32)
    cdf_val = 0.5 * (1.0 + lax.erf(z_val * INV_ROOT_TWO))
    hidden = (z_val * cdf_val).astype(jnp.bfloat16)
    slope = cdf_val + z_val * jnp.exp(-0.5 * z_val * z_val) * INV_ROOT_TWO_PI
    return hidden, slope


def block_backward(x_in, z_pre, grad_y, w_in, w_out):
    hidden, slope = gelu_pair(z_pre)
    w_out_grad = lax.dot_general(hidden, grad_y, CONTRACT_ROWS, preferred_element_type=jnp.float32).astype(jnp.bfloat16)
    grad_hidden = lax.dot_general(grad_y, w_out, CONTRACT_COLS, preferred_element_type=jnp.float32)
    grad_pre = (grad_hidden * slope).astype(jnp.bfloat16)
    w_in_grad = lax.dot_general(x_in, grad_pre, CONTRACT_ROWS, preferred_element_type=jnp.float32).astype(jnp.bfloat16)
    grad_x = (grad_y.astype(jnp.float32) + lax.dot_general(grad_pre, w_in, CONTRACT_COLS, preferred_element_type=jnp.float32)).astype(jnp.bfloat16)
    return w_out_grad, w_in_grad, grad_x


def reduce_grad(grad, group_size):
    part_sum = lax.psum_scatter(grad.astype(jnp.float32), AXES, scatter_dimension=0, tiled=True)
    return lax.all_gather(part_sum, AXES, axis=0, tiled=True)


def solution(mesh):
    group_size = mesh.shape['group']

    def device_step(x_one, z_one, x_two, z_two, grad_out, w1_in, w1_out, w2_in, w2_out):
        w2o_grad, w2i_grad, dx_two = block_backward(x_two, z_two, grad_out, w2_in, w2_out)
        sum_w2o = reduce_grad(w2o_grad, group_size)
        sum_w2i = reduce_grad(w2i_grad, group_size)
        w1o_grad, w1i_grad, dx_one = block_backward(x_one, z_one, dx_two, w1_in, w1_out)
        sum_w1o = reduce_grad(w1o_grad, group_size)
        sum_w1i = reduce_grad(w1i_grad, group_size)
        return sum_w2o, sum_w2i, sum_w1o, sum_w1i, dx_one

    row_spec = P(AXES, None)
    repl_spec = P()
    return jax.shard_map(
        device_step,
        mesh=mesh,
        in_specs=(row_spec, row_spec, row_spec, row_spec, row_spec, repl_spec, repl_spec, repl_spec, repl_spec),
        out_specs=(repl_spec, repl_spec, repl_spec, repl_spec, row_spec),
        check_vma=False,
    )
```

```python
import functools
import heapq
import math
import jax
import jax.numpy as jnp
from jax import lax
from jax.experimental import pallas as pl
from jax.experimental.pallas import tpu as pltpu
from jax.sharding import PartitionSpec as P

AXES = ('third', 'second', 'group')
INV_ROOT_TWO = math.sqrt(0.5)
INV_ROOT_TWO_PI = 1.0 / math.sqrt(2.0 * math.pi)
CONTRACT_ROWS = (((0,), (0,)), ((), ()))
CONTRACT_COLS = (((1,), (1,)), ((), ()))


def gelu_pair(z_pre):
    z_val = z_pre.astype(jnp.float32)
    cdf_val = 0.5 * (1.0 + lax.erf(z_val * INV_ROOT_TWO))
    hidden = (z_val * cdf_val).astype(jnp.bfloat16)
    slope = cdf_val + z_val * jnp.exp(-0.5 * z_val * z_val) * INV_ROOT_TWO_PI
    return hidden, slope


def block_backward(x_in, z_pre, grad_y, w_in, w_out):
    hidden, slope = gelu_pair(z_pre)
    w_out_grad = lax.dot_general(hidden, grad_y, CONTRACT_ROWS, preferred_element_type=jnp.float32).astype(jnp.bfloat16)
    grad_hidden = lax.dot_general(grad_y, w_out, CONTRACT_COLS, preferred_element_type=jnp.float32)
    grad_pre = (grad_hidden * slope).astype(jnp.bfloat16)
    w_in_grad = lax.dot_general(x_in, grad_pre, CONTRACT_ROWS, preferred_element_type=jnp.float32).astype(jnp.bfloat16)
    grad_x = (grad_y.astype(jnp.float32) + lax.dot_general(grad_pre, w_in, CONTRACT_COLS, preferred_element_type=jnp.float32)).astype(jnp.bfloat16)
    return w_out_grad, w_in_grad, grad_x


MESH = pl.DeviceIdType.MESH
CHUNKS = 2
STAGES = (('x', 'a', 'y', 'b'), ('y', 'a', 'x', 'b'))
LINK_NS_PER_BYTE = 1.0 / 46.6


def event_order(unit, width):
    chunks = [(g, j, c) for g in range(4) for j in range(CHUNKS) for c in range(2)]
    free = {'x': 0.0, 'y': 0.0, 'z': 0.0}
    heap = [(800.0 * (i + 1), i, 0) for i in range(len(chunks))]
    heapq.heapify(heap)
    order, now = [], 0.0
    while heap:
        when, i, stage = heapq.heappop(heap)
        now = max(now, when) + 300.0
        order.append((i, chunks[i], stage))
        if stage == 8:
            continue
        level = stage if stage < 4 else 7 - stage
        axis = STAGES[chunks[i][2]][level]
        link = 'z' if axis in 'ab' else axis
        size = (unit >> (level + 1)) * width * 4
        start = max(free[link], now)
        free[link] = start + size * LINK_NS_PER_BYTE
        heapq.heappush(heap, (free[link] + 2000.0, i, stage + 1))
    return chunks, order


def reduce_kernel(unit, width, *refs):
    grads, outs = refs[:4], refs[4:8]
    acc, own, rec_d, rec0, rec1, rec2, rec3, own_sem, send_sem, recv_sem, out_sem, free_sem = refs[8:]
    recs = (rec0, rec1, rec2, rec3)
    chunks, order = event_order(unit, width)
    group, second, third = lax.axis_index('group'), lax.axis_index('second'), lax.axis_index('third')
    core = group % 2
    peers = {
        'd': {'group': group + 1 - 2 * core},
        'x': {'group': (group + 2) % 4},
        'y': {'second': 1 - second},
        'a': {'third': third + 1 - 2 * (third % 2)},
        'b': {'third': (third + 2) % 4},
    }
    bits = {'x': group // 2, 'y': second, 'a': third % 2, 'b': third // 2}

    barrier = pltpu.get_barrier_semaphore()
    for peer in peers.values():
        pl.semaphore_signal(barrier, inc=1, device_id=peer, device_id_type=MESH)
    pl.semaphore_wait(barrier, len(peers))

    def window(ref, chunk, half):
        g, j, c = chunk
        if g % 2 == 0:
            return ref.at[pl.ds(half * 2 * unit + c * unit, unit), pl.ds(j * width, width)]
        return ref.at[pl.ds(0, unit), pl.ds(pl.multiple_of(half * 2 * unit + c * unit + j * width, 128), width)]

    def remote(src, dst, i, k, axis):
        return pltpu.make_async_remote_copy(
            src_ref=src, dst_ref=dst, send_sem=send_sem.at[i, k], recv_sem=recv_sem.at[i, k],
            device_id=peers[axis], device_id_type=MESH)

    own_copy, copies = {}, {}
    for i, chunk in enumerate(chunks):
        grad = grads[chunk[0]]
        own_copy[i] = pltpu.make_async_copy(window(grad, chunk, core), own.at[i], own_sem.at[i])
        own_copy[i].start()
        copies[i, 0] = remote(window(grad, chunk, 1 - core), rec_d.at[i], i, 0, 'd')
        copies[i, 0].start()

    def offsets(c):
        offs = [0]
        for k in range(4):
            offs.append(offs[-1] + bits[STAGES[c][k]] * (unit >> (k + 1)))
        return offs

    offs_of = (offsets(0), offsets(1))

    def rows_loop(count, fn):
        block = math.gcd(count, 32)

        @pl.loop(0, count // block)
        def _(t):
            fn(pl.multiple_of(t * block, 16), block)

    for i, chunk, stage in order:
        c = chunk[2]
        offs = offs_of[c]
        copies[i, stage].wait_recv()
        if stage == 0:
            own_copy[i].wait()

            def first(base, i=i):
                def fn(r, block):
                    rows = pl.ds(pl.multiple_of(base + r, 16), block)
                    acc[i, rows, :] = own[i, rows, :].astype(jnp.float32) + rec_d[i, rows, :].astype(jnp.float32)
                return fn

            bit = bits[STAGES[c][0]]
            rows_loop(unit // 2, first((1 - bit) * (unit // 2)))
        elif stage <= 4:
            keep = offs[stage]

            def add(r, block, i=i, keep=keep, rec=recs[stage - 1]):
                rows = pl.ds(pl.multiple_of(keep + r, 16), block)
                acc[i, rows, :] += rec[i, pl.ds(r, block), :]

            rows_loop(unit >> stage, add)
            copies[i, stage].wait_send()
            pl.semaphore_signal(free_sem.at[i, stage - 1], inc=1, device_id=peers[STAGES[c][stage - 1]], device_id_type=MESH)
        if stage < 4:
            half = unit >> (stage + 1)
            other = pl.multiple_of(offs[stage] + (1 - bits[STAGES[c][stage]]) * half, 16)
            copies[i, stage + 1] = remote(acc.at[i, pl.ds(other, half), :], recs[stage].at[i], i, stage + 1, STAGES[c][stage])
            copies[i, stage + 1].start()
            if stage == 0:
                rows_loop(unit // 2, first(bit * (unit // 2)))
        elif stage < 8:
            level = 7 - stage
            pl.semaphore_wait(free_sem.at[i, level], 1)
            rows = pl.ds(pl.multiple_of(offs[level + 1], 16), unit >> (level + 1))
            copies[i, stage + 1] = remote(acc.at[i, rows, :], acc.at[i, rows, :], i, stage + 1, STAGES[c][level])
            copies[i, stage + 1].start()
        else:
            dst = window(outs[chunk[0]], chunk, core)
            copies[i, 9] = remote(acc.at[i], dst, i, 9, 'd')
            copies[i, 9].start()
            pltpu.make_async_copy(acc.at[i], dst, out_sem.at[i]).start()

    for i, chunk in enumerate(chunks):
        for k in (0, 5, 6, 7, 8):
            copies[i, k].wait_send()
        copies[i, 9].wait()
        pltpu.make_async_copy(acc.at[i], window(outs[chunk[0]], chunk, core), out_sem.at[i]).wait()


def reduce_grads(grads):
    unit = grads[0].shape[1]
    width = unit // CHUNKS
    count = 4 * CHUNKS * 2
    any_spec = pl.BlockSpec(memory_space=pl.ANY)
    return pl.pallas_call(
        functools.partial(reduce_kernel, unit, width),
        name='reduce_grads',
        out_shape=[jax.ShapeDtypeStruct(grad.shape, jnp.float32) for grad in grads],
        in_specs=[any_spec] * 4,
        out_specs=[any_spec] * 4,
        scratch_shapes=[
            pltpu.VMEM((count, unit, width), jnp.float32),
            pltpu.VMEM((count, unit, width), jnp.bfloat16),
            pltpu.VMEM((count, unit, width), jnp.bfloat16),
            pltpu.VMEM((count, unit // 2, width), jnp.float32),
            pltpu.VMEM((count, unit // 4, width), jnp.float32),
            pltpu.VMEM((count, unit // 8, width), jnp.float32),
            pltpu.VMEM((count, unit // 16, width), jnp.float32),
            pltpu.SemaphoreType.DMA((count,)),
            pltpu.SemaphoreType.DMA((count, 10)),
            pltpu.SemaphoreType.DMA((count, 10)),
            pltpu.SemaphoreType.DMA((count,)),
            pltpu.SemaphoreType.REGULAR((count, 4)),
        ],
        compiler_params=pltpu.CompilerParams(
            collective_id=0, has_side_effects=True, vmem_limit_bytes=62 * 1024 * 1024),
    )(*grads)


def solution(mesh):
    def device_step(x_one, z_one, x_two, z_two, grad_out, w1_in, w1_out, w2_in, w2_out):
        w2o_grad, w2i_grad, dx_two = block_backward(x_two, z_two, grad_out, w2_in, w2_out)
        w1o_grad, w1i_grad, dx_one = block_backward(x_one, z_one, dx_two, w1_in, w1_out)
        sums = reduce_grads([w2o_grad, w2i_grad, w1o_grad, w1i_grad])
        return sums[0], sums[1], sums[2], sums[3], dx_one

    row_spec = P(AXES, None)
    repl_spec = P()
    return jax.shard_map(
        device_step,
        mesh=mesh,
        in_specs=(row_spec, row_spec, row_spec, row_spec, row_spec, repl_spec, repl_spec, repl_spec, repl_spec),
        out_specs=(repl_spec, repl_spec, repl_spec, repl_spec, row_spec),
        check_vma=False,
    )
```

```python
import functools
import heapq
import math
import jax
import jax.numpy as jnp
from jax import lax
from jax.experimental import pallas as pl
from jax.experimental.pallas import tpu as pltpu
from jax.sharding import PartitionSpec as P

AXES = ('third', 'second', 'group')
INV_ROOT_TWO = math.sqrt(0.5)
INV_ROOT_TWO_PI = 1.0 / math.sqrt(2.0 * math.pi)
CONTRACT_COLS = (((1,), (1,)), ((), ()))
CONTRACT_PLAIN = (((1,), (0,)), ((), ()))
MESH = pl.DeviceIdType.MESH
TILES = 12
PAIRS = TILES
CHUNKS = 2 * PAIRS
RING = 3
STAGES = (('x', 'a', 'y', 'b'), ('y', 'a', 'x', 'b'))
STEP_NS = 7000.0
NS_PER_BYTE = 1.0 / 44.0
HOP_NS = 2500.0
EVENT_NS = 400.0


def colour_of(i):
    return (i // 2 + i) % 2


def event_plan(unit, width):
    free = {'x': 0.0, 'y': 0.0, 'z': 0.0}
    arrive = []
    placed = {}
    tail = []

    def run(now, i, stage):
        now += EVENT_NS
        if stage < 8:
            level = stage if stage < 4 else 7 - stage
            axis = STAGES[colour_of(i)][level]
            link = 'z' if axis in 'ab' else axis
            size = (unit >> (level + 1)) * width * 4
            free[link] = max(free[link], now) + size * NS_PER_BYTE
            heapq.heappush(arrive, (free[link] + HOP_NS, i, stage + 1))
        return now

    now = 0.0
    for step in range(2 * TILES):
        for point in range(2):
            now += STEP_NS / 2
            events = []
            if point == 0 and step % 2 == 0 and step >= 2:
                events += [(step - 2, 0), (step - 1, 0)]
            while arrive and arrive[0][0] <= now:
                events.append(heapq.heappop(arrive)[1:])
            for i, stage in events:
                now = run(now, i, stage)
            placed[step, point] = events
    heapq.heappush(arrive, (now + 1000.0, CHUNKS - 2, 0))
    heapq.heappush(arrive, (now + 1000.0, CHUNKS - 1, 0))
    while arrive:
        when, i, stage = heapq.heappop(arrive)
        now = run(max(now, when), i, stage)
        tail.append((i, stage))
    return placed, tail


def step_kernel(*refs):
    x_two, z_two, grad_out, w2_in, w2_out, x_one, z_one, w1_in, w1_out = refs[:9]
    outs, dx_out = refs[9:13], refs[13]
    (acc, rec0, rec1, rec2, rec3, rec_d, tiles, dy, xv, dx_acc, zbuf, wo, wi, ht, dzt,
     send_sem, recv_sem, out_sem, load_sem, dy_sem, x_sem, dx_sem, free_sem, free_d) = refs[14:]
    recs = (rec0, rec1, rec2, rec3)
    unit, width = acc.shape[1], acc.shape[2]
    tokens = dy.shape[0]
    rows_block = min(256, tokens)
    placed, tail = event_plan(unit, width)
    group, second, third = lax.axis_index('group'), lax.axis_index('second'), lax.axis_index('third')
    core = group % 2
    peers = {
        'd': {'group': group + 1 - 2 * core},
        'x': {'group': (group + 2) % 4},
        'y': {'second': 1 - second},
        'a': {'third': third + 1 - 2 * (third % 2)},
        'b': {'third': (third + 2) % 4},
    }
    bits = {'x': group // 2, 'y': second, 'a': third % 2, 'b': third // 2}

    def loads(block, tile, slot):
        z_ref, wo_ref, wi_ref = ((z_two, w2_out, w2_in), (z_one, w1_out, w1_in))[block]
        span = pl.ds(pl.multiple_of(tile * unit, 128), unit)
        return (
            pltpu.make_async_copy(z_ref.at[:, span], zbuf.at[slot], load_sem.at[slot, 0]),
            pltpu.make_async_copy(wo_ref.at[span, :], wo.at[slot], load_sem.at[slot, 1]),
            pltpu.make_async_copy(wi_ref.at[:, span], wi.at[slot], load_sem.at[slot, 2]),
        )

    dy_load = pltpu.make_async_copy(grad_out, dy, dy_sem)
    dy_load.start()
    for copy in loads(0, 0, 0):
        copy.start()
    pltpu.make_async_copy(x_two, xv, x_sem).start()

    barrier = pltpu.get_barrier_semaphore()
    for peer in peers.values():
        pl.semaphore_signal(barrier, inc=1, device_id=peer, device_id_type=MESH)
    pl.semaphore_wait(barrier, len(peers))

    def remote(src, dst, i, k, axis):
        return pltpu.make_async_remote_copy(
            src_ref=src, dst_ref=dst, send_sem=send_sem.at[i, k], recv_sem=recv_sem.at[i, k],
            device_id=peers[axis], device_id_type=MESH)

    def offsets(c):
        offs = [0]
        for k in range(4):
            offs.append(offs[-1] + bits[STAGES[c][k]] * (unit >> (k + 1)))
        return offs

    offs_of = (offsets(0), offsets(1))

    def rows_loop(count, fn):
        block = math.gcd(count, 16)

        @pl.loop(0, count // block)
        def _(t):
            fn(pl.multiple_of(t * block, 8), block)

    def pair_copy(q, kind, i):
        slot = q % RING
        return remote(tiles.at[slot, kind, 1 - core], rec_d.at[slot, kind], i, 0, 'd')

    def out_copies(i):
        block, q, kind = i // TILES, (i // 2) % (TILES // 2), i % 2
        dst = outs[2 * block + kind].at[pl.ds(pl.multiple_of((2 * q + core) * unit, 16), unit), :]
        return remote(acc.at[i], dst, i, 9, 'd'), pltpu.make_async_copy(acc.at[i], dst, out_sem.at[i])

    def level_copy(i, stage):
        axes, offs = STAGES[colour_of(i)], offs_of[colour_of(i)]
        if stage < 4:
            half = unit >> (stage + 1)
            other = pl.multiple_of(offs[stage] + (1 - bits[axes[stage]]) * half, 8)
            return remote(acc.at[i, pl.ds(other, half), :], recs[stage].at[i], i, stage + 1, axes[stage])
        level = 7 - stage
        rows = pl.ds(pl.multiple_of(offs[level + 1], 8), unit >> (level + 1))
        return remote(acc.at[i, rows, :], acc.at[i, rows, :], i, stage + 1, axes[level])

    def event(i, stage):
        axes, offs = STAGES[colour_of(i)], offs_of[colour_of(i)]
        if stage == 0:
            q, kind = i // 2, i % 2
            slot = q % RING
            got = pair_copy(q, kind, i)
            got.wait_recv()

            def first(base):
                def fn(r, block):
                    rows = pl.ds(pl.multiple_of(base + r, 8), block)
                    acc[i, rows, :] = tiles[slot, kind, core, rows, :].astype(jnp.float32) + rec_d[slot, kind, rows, :].astype(jnp.float32)
                return fn

            bit = bits[axes[0]]
            rows_loop(unit // 2, first((1 - bit) * (unit // 2)))
            level_copy(i, 0).start()
            rows_loop(unit // 2, first(bit * (unit // 2)))
            got.wait_send()
            if i + 2 * RING < CHUNKS:
                pl.semaphore_signal(free_d.at[i], inc=1, device_id=peers['d'], device_id_type=MESH)
            return
        arrived = level_copy(i, stage - 1)
        arrived.wait_recv()
        if stage <= 4:
            keep = offs[stage]

            def add(r, block):
                rows = pl.ds(pl.multiple_of(keep + r, 8), block)
                acc[i, rows, :] += recs[stage - 1][i, pl.ds(r, block), :]

            rows_loop(unit >> stage, add)
        if 4 <= stage < 8:
            if stage == 4:
                arrived.wait_send()
                pl.semaphore_signal(free_sem.at[i, 3], inc=1, device_id=peers[axes[3]], device_id_type=MESH)
            pl.semaphore_wait(free_sem.at[i, 7 - stage], 1)
            level_copy(i, stage).start()
        elif stage < 4:
            level_copy(i, stage).start()
            arrived.wait_send()
            pl.semaphore_signal(free_sem.at[i, stage - 1], inc=1, device_id=peers[axes[stage - 1]], device_id_type=MESH)
        else:
            for copy in out_copies(i):
                copy.start()

    def run_events(step, point):
        span = 4
        for lo in range(0, 2 * TILES, span):
            if any(placed[k, point] for k in range(lo, lo + span)):
                @pl.when((step >= lo) & (step < lo + span))
                def _(lo=lo):
                    for k in range(lo, lo + span):
                        if placed[k, point]:
                            @pl.when(step == k)
                            def _(k=k):
                                for i, stage in placed[k, point]:
                                    event(i, stage)

    dy_load.wait()

    @pl.loop(0, tokens // rows_block)
    def _(r):
        rows = pl.ds(pl.multiple_of(r * rows_block, 16), rows_block)
        dx_acc[rows, :] = dy[rows, :].astype(jnp.float32)

    @pl.loop(0, 2 * TILES)
    def _(step):
        slot = step % 2
        for copy in loads(0, 0, slot):
            copy.wait()

        @pl.when(step < TILES - 1)
        def _():
            for copy in loads(0, step + 1, 1 - slot):
                copy.start()

        @pl.when((step >= TILES - 1) & (step < 2 * TILES - 1))
        def _():
            for copy in loads(1, step + 1 - TILES, 1 - slot):
                copy.start()

        @pl.loop(0, tokens // rows_block)
        def _(r):
            rows = pl.ds(pl.multiple_of(r * rows_block, 128), rows_block)
            z_val = zbuf[slot, rows, :].astype(jnp.float32)
            cdf_val = 0.5 * (1.0 + lax.erf(z_val * INV_ROOT_TWO))
            ht[:, rows] = (z_val * cdf_val).astype(jnp.bfloat16).T
            slope = cdf_val + z_val * jnp.exp(-0.5 * z_val * z_val) * INV_ROOT_TWO_PI
            grad_hidden = lax.dot_general(dy[rows, :], wo[slot], CONTRACT_COLS, preferred_element_type=jnp.float32)
            grad_pre = (grad_hidden * slope).astype(jnp.bfloat16)
            dzt[:, rows] = grad_pre.T
            dx_acc[rows, :] += lax.dot_general(grad_pre, wi[slot], CONTRACT_COLS, preferred_element_type=jnp.float32)

        run_events(step, 0)

        @pl.when((step == 0) | (step == TILES))
        def _():
            pltpu.make_async_copy(x_two, xv, x_sem).wait()

        pair = (step // 2) % RING
        tiles[pair, 0, slot] = lax.dot_general(ht[...], dy[...], CONTRACT_PLAIN, preferred_element_type=jnp.float32).astype(jnp.bfloat16)
        tiles[pair, 1, slot] = lax.dot_general(dzt[...], xv[...], CONTRACT_PLAIN, preferred_element_type=jnp.float32).astype(jnp.bfloat16)

        @pl.when((step == TILES - 1) | (step == 2 * TILES - 1))
        def _():
            @pl.loop(0, tokens // rows_block)
            def _(r):
                rows = pl.ds(pl.multiple_of(r * rows_block, 16), rows_block)
                grad_x = dx_acc[rows, :].astype(jnp.bfloat16)
                dy[rows, :] = grad_x
                dx_acc[rows, :] = grad_x.astype(jnp.float32)

        @pl.when(step == TILES - 1)
        def _():
            pltpu.make_async_copy(x_one, xv, x_sem).start()

        @pl.when(slot == 1)
        def _():
            q = step // 2
            for kind in range(2):
                i = 2 * q + kind

                @pl.when(q >= RING)
                def _():
                    pl.semaphore_wait(free_d.at[i - 2 * RING], 1)

                pair_copy(q, kind, i).start()

        run_events(step, 1)

    dx_store = pltpu.make_async_copy(dy, dx_out, dx_sem)
    dx_store.start()
    for i, stage in tail:
        event(i, stage)
    dx_store.wait()
    for i in range(CHUNKS):
        for stage in range(4, 8):
            level_copy(i, stage).wait_send()
        far, near = out_copies(i)
        far.wait()
        near.wait()


def backward_and_reduce(x_one, z_one, x_two, z_two, grad_out, w1_in, w1_out, w2_in, w2_out):
    tokens, width = x_one.shape
    hidden = z_one.shape[1]
    unit = hidden // TILES
    any_spec = pl.BlockSpec(memory_space=pl.ANY)
    bf16, f32 = jnp.bfloat16, jnp.float32
    return pl.pallas_call(
        step_kernel,
        name='backward_and_reduce',
        out_shape=[jax.ShapeDtypeStruct((hidden, width), f32)] * 4 + [jax.ShapeDtypeStruct((tokens, width), bf16)],
        in_specs=[any_spec] * 9,
        out_specs=[any_spec] * 5,
        scratch_shapes=[
            pltpu.VMEM((CHUNKS, unit, width), f32),
            pltpu.VMEM((CHUNKS, unit // 2, width), f32),
            pltpu.VMEM((CHUNKS, unit // 4, width), f32),
            pltpu.VMEM((CHUNKS, unit // 8, width), f32),
            pltpu.VMEM((CHUNKS, unit // 16, width), f32),
            pltpu.VMEM((RING, 2, unit, width), bf16),
            pltpu.VMEM((RING, 2, 2, unit, width), bf16),
            pltpu.VMEM((tokens, width), bf16),
            pltpu.VMEM((tokens, width), bf16),
            pltpu.VMEM((tokens, width), f32),
            pltpu.VMEM((2, tokens, unit), bf16),
            pltpu.VMEM((2, unit, width), bf16),
            pltpu.VMEM((2, width, unit), bf16),
            pltpu.VMEM((unit, tokens), bf16),
            pltpu.VMEM((unit, tokens), bf16),
            pltpu.SemaphoreType.DMA((CHUNKS, 10)),
            pltpu.SemaphoreType.DMA((CHUNKS, 10)),
            pltpu.SemaphoreType.DMA((CHUNKS,)),
            pltpu.SemaphoreType.DMA((2, 3)),
            pltpu.SemaphoreType.DMA,
            pltpu.SemaphoreType.DMA,
            pltpu.SemaphoreType.DMA,
            pltpu.SemaphoreType.REGULAR((CHUNKS, 4)),
            pltpu.SemaphoreType.REGULAR((CHUNKS,)),
        ],
        compiler_params=pltpu.CompilerParams(
            collective_id=0, has_side_effects=True, vmem_limit_bytes=67043328),
    )(x_two, z_two, grad_out, w2_in, w2_out, x_one, z_one, w1_in, w1_out)


def solution(mesh):
    def device_step(*args):
        w2o, w2i_t, w1o, w1i_t, dx_one = backward_and_reduce(*args)
        return w2o, w2i_t.T, w1o, w1i_t.T, dx_one

    row_spec = P(AXES, None)
    repl_spec = P()
    return jax.shard_map(
        device_step,
        mesh=mesh,
        in_specs=(row_spec, row_spec, row_spec, row_spec, row_spec, repl_spec, repl_spec, repl_spec, repl_spec),
        out_specs=(repl_spec, repl_spec, repl_spec, repl_spec, row_spec),
        check_vma=False,
    )
```

```python
import functools
import heapq
import math
import jax
import jax.numpy as jnp
from jax import lax
from jax.experimental import pallas as pl
from jax.experimental.pallas import tpu as pltpu
from jax.sharding import PartitionSpec as P

AXES = ('third', 'second', 'group')
INV_ROOT_TWO = math.sqrt(0.5)
INV_ROOT_TWO_PI = 1.0 / math.sqrt(2.0 * math.pi)
CONTRACT_COLS = (((1,), (1,)), ((), ()))
CONTRACT_PLAIN = (((1,), (0,)), ((), ()))
MESH = pl.DeviceIdType.MESH
TILES = 12
PAIRS = TILES
CHUNKS = 2 * PAIRS
RING = 3
STEP_NS = 5500.0
NS_PER_BYTE = 1.0 / 45.0
HOP_NS = 2200.0
EVENT_NS = 300.0
POINTS = 2


def event_plan(unit, width):
    free = {}
    arrive = []
    placed = {}
    tail = []
    row = width * 4 * NS_PER_BYTE
    quarter = unit // 8

    def run(now, q, stage):
        now += EVENT_NS
        if stage == 0 or stage == 9:
            sends = [('plane', unit // 2)]
        elif stage <= 3:
            sends = [(stage, 2 * (4 - stage) * quarter)]
        elif stage <= 5:
            sends = [('plane', quarter // 2)]
        elif stage <= 8:
            sends = [(k, 2 * quarter) for k in range(stage - 5, 4)]
        else:
            return now
        for link, rows in sends:
            free[link] = max(free.get(link, 0.0), now) + rows * row
        heapq.heappush(arrive, (max(free[link] for link, _ in sends) + HOP_NS, q, stage + 1))
        return now

    now = 0.0
    for step in range(2 * TILES):
        for point in range(POINTS):
            now += STEP_NS / POINTS
            events = []
            if point == 0 and step % 2 == 0 and step >= 2:
                events.append((step // 2 - 1, 0))
            while arrive and arrive[0][0] <= now:
                events.append(heapq.heappop(arrive)[1:])
            for q, stage in events:
                now = run(now, q, stage)
            placed[step, point] = events
    heapq.heappush(arrive, (now + 1000.0, PAIRS - 1, 0))
    while arrive:
        when, q, stage = heapq.heappop(arrive)
        now = run(max(now, when), q, stage)
        tail.append((q, stage))
    return placed, tail


def step_kernel(*refs):
    x_two, z_two, grad_out, w2_in, w2_out, x_one, z_one, w1_in, w1_out = refs[:9]
    outs, dx_out = refs[9:13], refs[13]
    (acc, rec_first, rec_line, rec_last, rec_d, tiles, dy, xv, dx_acc, zbuf, wo, wi, ht, dzt,
     send_sem, recv_sem, out_sem, load_sem, dy_sem, x_sem, dx_sem, free_sem, free_line, free_d) = refs[14:]
    unit, width = acc.shape[1], acc.shape[2]
    tokens = dy.shape[0]
    rows_block = min(256, tokens)
    placed, tail = event_plan(unit, width)
    group, second, third = lax.axis_index('group'), lax.axis_index('second'), lax.axis_index('third')
    core, x_bit = lax.rem(group, 2), group // 2
    half, quarter, piece = unit // 2, unit // 8, unit // 16
    peer_core = {'group': group + 1 - 2 * core}
    peer_x = {'group': group + 2 - 4 * x_bit}
    peer_y = {'second': 1 - second}
    peer_up, peer_down = {'third': lax.rem(third + 1, 4)}, {'third': lax.rem(third + 3, 4)}
    at = [third == place for place in range(4)]
    above, below = [third >= hop for hop in range(4)], [third <= 3 - hop for hop in range(4)]
    can_up, can_down = below[1], above[1]
    turn = [lax.rem(third + c, 4) * quarter for c in range(4)]

    def loads(block, tile, slot):
        z_ref, wo_ref, wi_ref = ((z_two, w2_out, w2_in), (z_one, w1_out, w1_in))[block]
        span = pl.ds(pl.multiple_of(tile * unit, 128), unit)
        return (
            pltpu.make_async_copy(z_ref.at[:, span], zbuf.at[slot], load_sem.at[slot, 0]),
            pltpu.make_async_copy(wo_ref.at[span, :], wo.at[slot], load_sem.at[slot, 1]),
            pltpu.make_async_copy(wi_ref.at[:, span], wi.at[slot], load_sem.at[slot, 2]),
        )

    dy_load = pltpu.make_async_copy(grad_out, dy, dy_sem)
    dy_load.start()
    for copy in loads(0, 0, 0):
        copy.start()
    pltpu.make_async_copy(x_two, xv, x_sem).start()

    barrier = pltpu.get_barrier_semaphore()
    for peer in (peer_core, peer_x, peer_y, peer_up, peer_down):
        pl.semaphore_signal(barrier, inc=1, device_id=peer, device_id_type=MESH)
    pl.semaphore_wait(barrier, 5)

    def remote(src, dst, i, k, peer):
        return pltpu.make_async_remote_copy(
            src_ref=src, dst_ref=dst, send_sem=send_sem.at[i, k], recv_sem=recv_sem.at[i, k],
            device_id=peer, device_id_type=MESH)

    def rows_loop(count, fn):
        block = math.gcd(count, 16)

        @pl.loop(0, count // block)
        def _(t):
            fn(pl.multiple_of(t * block, 8), block)

    def pair_copy(q, kind, i):
        slot = q % RING
        return remote(tiles.at[slot, kind, 1 - core], rec_d.at[slot, kind], i, 0, peer_core)

    def out_copies(i, kind, tile):
        block = tile // TILES
        out = outs[2 * block + kind]
        span = pl.ds(pl.multiple_of((tile - TILES * block + core) * unit, 128), unit)
        copies = []
        if kind == 0:
            pairs = [(acc.at[i], out.at[span, :])]
        else:
            pairs = [(acc.at[i, :, pl.ds(b * unit, unit)], out.at[pl.ds(b * unit, unit), span]) for b in range(width // unit)]
        for b, (src, dst) in enumerate(pairs):
            copies += [remote(src, dst, i, 13 + b, peer_core), pltpu.make_async_copy(src, dst, out_sem.at[i, b])]
        return copies

    class Chunk:
        def __init__(self, q, kind):
            self.q, self.kind, self.i = q, kind, 2 * q + kind
            colour = lax.rem(q + kind, 2)
            self.first_bit = x_bit + colour * (second - x_bit)
            self.last_bit = second + colour * (x_bit - second)
            self.first_peer = {'group': group + (1 - colour) * (2 - 4 * x_bit), 'second': second + colour * (1 - 2 * second)}
            self.last_peer = {'group': group + colour * (2 - 4 * x_bit), 'second': second + (1 - colour) * (1 - 2 * second)}
            self.kept = pl.multiple_of(self.first_bit * half, 8)
            self.other = pl.multiple_of(half - self.kept, 8)

        def span(self, row, count):
            return acc.at[self.i, pl.ds(pl.multiple_of(row, 8), count), :]

        def first(self):
            slot = 2 * (self.q % (PAIRS // 2)) + self.kind
            return remote(self.span(self.other, half), rec_first.at[slot], self.i, 1, self.first_peer)

        def up(self, place):
            rows = (3 - place) * quarter
            return remote(self.span(self.kept + (place + 1) * quarter, rows), rec_line.at[self.i, pl.ds(0, rows), :], self.i, 2, peer_up)

        def down(self, place):
            rows = place * quarter
            dst = rec_line.at[self.i, pl.ds((5 - place) * quarter, rows), :]
            return remote(self.span(self.kept, rows), dst, self.i, 3, peer_down)

        def mine(self):
            return self.kept + turn[0] + self.last_bit * piece

        def last(self):
            other = self.kept + turn[0] + (1 - self.last_bit) * piece
            return remote(self.span(other, piece), rec_last.at[self.i], self.i, 4, self.last_peer)

        def last_back(self):
            ref = self.span(self.mine(), piece)
            return remote(ref, ref, self.i, 5, self.last_peer)

        def spread_up(self, hop, arriving=0):
            ref = self.span(self.kept + turn[(5 - hop - arriving) % 4], quarter)
            return remote(ref, ref, self.i, 5 + hop, peer_up)

        def spread_down(self, hop, arriving=0):
            ref = self.span(self.kept + turn[(hop - 1 + arriving) % 4], quarter)
            return remote(ref, ref, self.i, 8 + hop, peer_down)

        def first_back(self):
            ref = self.span(self.kept, half)
            return remote(ref, ref, self.i, 12, self.first_peer)

    def signal(sem, peer):
        pl.semaphore_signal(sem, inc=1, device_id=peer, device_id_type=MESH)

    def add_rows(i, base, rec, rec_index, rec_base, count):
        def add(r, block):
            rows = pl.ds(pl.multiple_of(base + r, 8), block)
            acc[i, rows, :] += rec[rec_index, pl.ds(pl.multiple_of(rec_base + r, 8), block), :]

        rows_loop(count, add)

    def chunk_event(q, kind, stage):
        chunk = Chunk(q, kind)
        i, kept = chunk.i, chunk.kept
        if stage == 0:
            slot = q % RING
            got = pair_copy(q, kind, i)
            got.wait_recv()

            def first(base):
                def fn(r, block):
                    rows = pl.ds(pl.multiple_of(base + r, 8), block)
                    acc[i, rows, :] = tiles[slot, kind, core, rows, :].astype(jnp.float32) + rec_d[slot, kind, rows, :].astype(jnp.float32)
                return fn

            rows_loop(half, first(chunk.other))
            if q >= PAIRS // 2:
                pl.semaphore_wait(free_sem.at[i - PAIRS, 2], 1)
            chunk.first().start()
            rows_loop(half, first(kept))
            got.wait_send()
            if q + RING < PAIRS:
                signal(free_d.at[i], peer_core)
        elif stage == 1:
            got = chunk.first()
            got.wait_recv()
            add_rows(i, kept, rec_first, 2 * (q % (PAIRS // 2)) + kind, 0, half)

            @pl.when(at[0])
            def _():
                chunk.up(0).start()

            @pl.when(at[3])
            def _():
                chunk.down(3).start()

            if q < PAIRS // 2:
                signal(free_sem.at[i, 2], chunk.first_peer)
            got.wait_send()
            signal(free_sem.at[i, 0], chunk.first_peer)
        elif stage <= 4:
            hop = stage - 1

            @pl.when(at[hop])
            def _():
                chunk.up(hop - 1).wait_recv()
                add_rows(i, kept + hop * quarter, rec_line, i, 0, (4 - hop) * quarter)
                if hop < 3:
                    chunk.up(hop).start()

            @pl.when(at[3 - hop])
            def _():
                chunk.down(4 - hop).wait_recv()
                add_rows(i, kept, rec_line, i, (1 + hop) * quarter, (4 - hop) * quarter)
                if hop < 3:
                    chunk.down(3 - hop).start()

            if hop == 3:
                chunk.last().start()
        elif stage == 5:
            got = chunk.last()
            got.wait_recv()
            add_rows(i, chunk.mine(), rec_last, i, 0, piece)
            got.wait_send()
            signal(free_sem.at[i, 1], chunk.last_peer)
            pl.semaphore_wait(free_sem.at[i, 1], 1)
            chunk.last_back().start()
            for place in range(4):
                @pl.when(at[place])
                def _(place=place):
                    if place < 3:
                        chunk.up(place).wait_send()
                        signal(free_line.at[i, 0], peer_up)
                    if place > 0:
                        chunk.down(place).wait_send()
                        signal(free_line.at[i, 1], peer_down)
        elif stage == 6:
            chunk.last_back().wait_recv()

            @pl.when(can_up)
            def _():
                pl.semaphore_wait(free_line.at[i, 1], 1)
                chunk.spread_up(1).start()

            @pl.when(can_down)
            def _():
                pl.semaphore_wait(free_line.at[i, 0], 1)
                chunk.spread_down(1).start()
        elif stage <= 9:
            hop = stage - 6

            @pl.when(above[hop])
            def _():
                chunk.spread_up(hop, 1).wait_recv()
                if hop < 3:
                    @pl.when(can_up)
                    def _():
                        chunk.spread_up(hop + 1).start()

            @pl.when(below[hop])
            def _():
                chunk.spread_down(hop, 1).wait_recv()
                if hop < 3:
                    @pl.when(can_down)
                    def _():
                        chunk.spread_down(hop + 1).start()

            if hop == 3:
                pl.semaphore_wait(free_sem.at[i, 0], 1)
                chunk.first_back().start()
        else:
            chunk.first_back().wait_recv()

    def event(q, stage):
        @pl.loop(0, 2)
        def _(kind):
            chunk_event(q, kind, stage)

        if stage == 10:
            for kind in range(2):
                for copy in out_copies(2 * q + kind, kind, 2 * q):
                    copy.start()

    def run_events(step, point):
        span = 4
        for lo in range(0, 2 * TILES, span):
            if any(placed[k, point] for k in range(lo, lo + span)):
                @pl.when((step >= lo) & (step < lo + span))
                def _(lo=lo):
                    for k in range(lo, lo + span):
                        if placed[k, point]:
                            @pl.when(step == k)
                            def _(k=k):
                                for q, stage in placed[k, point]:
                                    event(q, stage)

    dy_load.wait()

    @pl.loop(0, tokens // rows_block)
    def _(r):
        rows = pl.ds(pl.multiple_of(r * rows_block, 16), rows_block)
        dx_acc[rows, :] = dy[rows, :].astype(jnp.float32)

    @pl.loop(0, 2 * TILES)
    def _(step):
        slot = step % 2
        for copy in loads(0, 0, slot):
            copy.wait()

        @pl.when(step < TILES - 1)
        def _():
            for copy in loads(0, step + 1, 1 - slot):
                copy.start()

        @pl.when((step >= TILES - 1) & (step < 2 * TILES - 1))
        def _():
            for copy in loads(1, step + 1 - TILES, 1 - slot):
                copy.start()

        @pl.loop(0, tokens // rows_block)
        def _(r):
            rows = pl.ds(pl.multiple_of(r * rows_block, 128), rows_block)
            z_val = zbuf[slot, rows, :].astype(jnp.float32)
            cdf_val = 0.5 * (1.0 + lax.erf(z_val * INV_ROOT_TWO))
            ht[:, rows] = (z_val * cdf_val).astype(jnp.bfloat16).T
            slope = cdf_val + z_val * jnp.exp(-0.5 * z_val * z_val) * INV_ROOT_TWO_PI
            grad_hidden = lax.dot_general(dy[rows, :], wo[slot], CONTRACT_COLS, preferred_element_type=jnp.float32)
            grad_pre = (grad_hidden * slope).astype(jnp.bfloat16)
            dzt[:, rows] = grad_pre.T
            dx_acc[rows, :] += lax.dot_general(grad_pre, wi[slot], CONTRACT_COLS, preferred_element_type=jnp.float32)

        run_events(step, 0)

        @pl.when((step == 0) | (step == TILES))
        def _():
            pltpu.make_async_copy(x_two, xv, x_sem).wait()

        pair = (step // 2) % RING
        tiles[pair, 0, slot] = lax.dot_general(ht[...], dy[...], CONTRACT_PLAIN, preferred_element_type=jnp.float32).astype(jnp.bfloat16)
        for b in range(width // unit):
            cols = pl.ds(b * unit, unit)
            tile = lax.dot_general(dzt[...], xv[:, cols], CONTRACT_PLAIN, preferred_element_type=jnp.float32)
            tiles[pair, 1, slot, :, cols] = tile.T.astype(jnp.bfloat16)

        @pl.when((step == TILES - 1) | (step == 2 * TILES - 1))
        def _():
            @pl.loop(0, tokens // rows_block)
            def _(r):
                rows = pl.ds(pl.multiple_of(r * rows_block, 16), rows_block)
                grad_x = dx_acc[rows, :].astype(jnp.bfloat16)
                dy[rows, :] = grad_x
                dx_acc[rows, :] = grad_x.astype(jnp.float32)

        @pl.when(step == TILES - 1)
        def _():
            pltpu.make_async_copy(x_one, xv, x_sem).start()

        @pl.when(slot == 1)
        def _():
            q = step // 2
            for kind in range(2):
                i = 2 * q + kind

                @pl.when(q >= RING)
                def _():
                    pl.semaphore_wait(free_d.at[i - 2 * RING], 1)

                pair_copy(q, kind, i).start()

        run_events(step, 1)

    dx_store = pltpu.make_async_copy(dy, dx_out, dx_sem)
    dx_store.start()
    for q, stage in tail:
        event(q, stage)
    dx_store.wait()

    @pl.loop(0, PAIRS)
    def _(q):
        for kind in range(2):
            chunk = Chunk(q, kind)
            chunk.last_back().wait_send()
            for hop in range(1, 4):
                @pl.when(above[hop - 1] & can_up)
                def _(chunk=chunk, hop=hop):
                    chunk.spread_up(hop).wait_send()

                @pl.when(below[hop - 1] & can_down)
                def _(chunk=chunk, hop=hop):
                    chunk.spread_down(hop).wait_send()
            chunk.first_back().wait_send()

    for q in range(PAIRS):
        for kind in range(2):
            for copy in out_copies(2 * q + kind, kind, 2 * q):
                copy.wait()


def backward_and_reduce(x_one, z_one, x_two, z_two, grad_out, w1_in, w1_out, w2_in, w2_out):
    tokens, width = x_one.shape
    hidden = z_one.shape[1]
    unit = hidden // TILES
    any_spec = pl.BlockSpec(memory_space=pl.ANY)
    bf16, f32 = jnp.bfloat16, jnp.float32
    return pl.pallas_call(
        step_kernel,
        name='backward_and_reduce',
        out_shape=[jax.ShapeDtypeStruct((hidden, width), f32), jax.ShapeDtypeStruct((width, hidden), f32)] * 2 + [jax.ShapeDtypeStruct((tokens, width), bf16)],
        in_specs=[any_spec] * 9,
        out_specs=[any_spec] * 5,
        scratch_shapes=[
            pltpu.VMEM((CHUNKS, unit, width), f32),
            pltpu.VMEM((PAIRS, unit // 2, width), f32),
            pltpu.VMEM((CHUNKS, 5 * unit // 8, width), f32),
            pltpu.VMEM((CHUNKS, unit // 16, width), f32),
            pltpu.VMEM((RING, 2, unit, width), bf16),
            pltpu.VMEM((RING, 2, 2, unit, width), bf16),
            pltpu.VMEM((tokens, width), bf16),
            pltpu.VMEM((tokens, width), bf16),
            pltpu.VMEM((tokens, width), f32),
            pltpu.VMEM((2, tokens, unit), bf16),
            pltpu.VMEM((2, unit, width), bf16),
            pltpu.VMEM((2, width, unit), bf16),
            pltpu.VMEM((unit, tokens), bf16),
            pltpu.VMEM((unit, tokens), bf16),
            pltpu.SemaphoreType.DMA((CHUNKS, 13 + width // unit)),
            pltpu.SemaphoreType.DMA((CHUNKS, 13 + width // unit)),
            pltpu.SemaphoreType.DMA((CHUNKS, width // unit)),
            pltpu.SemaphoreType.DMA((2, 3)),
            pltpu.SemaphoreType.DMA,
            pltpu.SemaphoreType.DMA,
            pltpu.SemaphoreType.DMA,
            pltpu.SemaphoreType.REGULAR((CHUNKS, 3)),
            pltpu.SemaphoreType.REGULAR((CHUNKS, 2)),
            pltpu.SemaphoreType.REGULAR((CHUNKS,)),
        ],
        compiler_params=pltpu.CompilerParams(
            collective_id=0, has_side_effects=True, vmem_limit_bytes=67043328),
    )(x_two, z_two, grad_out, w2_in, w2_out, x_one, z_one, w1_in, w1_out)


def solution(mesh):
    def device_step(*args):
        return tuple(backward_and_reduce(*args))

    row_spec = P(AXES, None)
    repl_spec = P()
    return jax.shard_map(
        device_step,
        mesh=mesh,
        in_specs=(row_spec, row_spec, row_spec, row_spec, row_spec, repl_spec, repl_spec, repl_spec, repl_spec),
        out_specs=(repl_spec, repl_spec, repl_spec, repl_spec, row_spec),
        check_vma=False,
    )
```

```python
import functools
import math
import jax
import jax.numpy as jnp
from jax import lax
from jax.experimental import pallas as pl
from jax.experimental.pallas import tpu as pltpu
from jax.sharding import PartitionSpec as P

AXES = ('third', 'second', 'group')
INV_ROOT_TWO = math.sqrt(0.5)
INV_ROOT_TWO_PI = 1.0 / math.sqrt(2.0 * math.pi)
CONTRACT_COLS = (((1,), (1,)), ((), ()))
CONTRACT_PLAIN = (((1,), (0,)), ((), ()))
MESH = pl.DeviceIdType.MESH
TILES = 12
PAIRS = TILES
CHUNKS = 2 * PAIRS
RING = 3
POINTS = 4
ORDER = (
    -1, -1, -1, -1, -1, -1, -1, -1, -1, 0, -1, -1, -1, -1, -1, -1, 1, -1, -1, 11, -1, -1, -1, -1,
    -1, 2, 12, -1, -1, -1, 22, -1, -1, 3, -1, -1, -1, 4, 13, 23, -1, 5, -1, -1, 33, 6, -1, -1,
    14, -1, -1, 24, -1, 34, 15, -1, 7, -1, -1, 16, 44, 25, 17, -1, -1, -1, 35, 8, 26, -1, 45, 18,
    27, -1, 9, -1, 28, -1, -1, 36, 55, 19, -1, 46, -1, -1, -1, 29, 37, 20, -1, 56, 38, 47, -1, -1,
    -1, 30, 66, -1, 39, -1, 48, -1, 31, 57, -1, -1, 67, 40, -1, -1, 10, 49, 58, 21, 77, -1, 50, -1,
    41, -1, 68, 59, -1, -1, 51, 78, 60, 42, -1, -1, -1, 32, 69, -1, 88, 52, 61, -1, -1, 79, -1, -1,
    70, 53, -1, 62, 89, -1, -1, 80, 71, -1, 99, 63, -1, 72, -1, -1, 90, 81, -1, 64, -1, 100, 73, -1,
    -1, 82, 91, 110, -1, 83, -1, 92, -1, 74, 101, -1, -1, 84, 111, 93, 75, -1, 54, 94, -1, -1, 85, 102,
    121, 112, 95, 103, 113, 122, 104, 114, 96, 105, 115, 65, 86, 116, 76, 123, 97, 106, 117, 124, 125, 107, 126, 108,
    127, 87, 118, 128, 119, 129, 130, 98, 43, 109, 120, 131,
)


def event_plan():
    placed = {(step, point): [] for step in range(2 * TILES) for point in range(POINTS)}
    quarters, tail = 0, []
    for entry in ORDER:
        if entry < 0:
            quarters += 1
        elif quarters < 2 * TILES * POINTS:
            placed[(quarters - 1) // POINTS, (quarters - 1) % POINTS].append(divmod(entry, 11))
        else:
            tail.append(divmod(entry, 11))
    return placed, tail


def step_kernel(*refs):
    x_two, z_two, grad_out, w2_in, w2_out, x_one, z_one, w1_in, w1_out = refs[:9]
    outs, dx_out = refs[9:13], refs[13]
    (acc, rec_first, rec_line, rec_last, rec_d, tiles, dy, xv, dx_acc, zbuf, wo, wi, ht, dzt,
     send_sem, recv_sem, out_sem, load_sem, dy_sem, x_sem, dx_sem, free_sem, free_line, free_d) = refs[14:]
    unit, width = acc.shape[1], acc.shape[2]
    tokens = dy.shape[0]
    rows_block = min(256, tokens)
    placed, tail = event_plan()
    group, second, third = lax.axis_index('group'), lax.axis_index('second'), lax.axis_index('third')
    core, x_bit = lax.rem(group, 2), group // 2
    half, quarter, piece = unit // 2, unit // 8, unit // 16
    peer_core = {'group': group + 1 - 2 * core}
    peer_x = {'group': group + 2 - 4 * x_bit}
    peer_y = {'second': 1 - second}
    peer_up, peer_down = {'third': lax.rem(third + 1, 4)}, {'third': lax.rem(third + 3, 4)}
    at = [third == place for place in range(4)]
    above, below = [third >= hop for hop in range(4)], [third <= 3 - hop for hop in range(4)]
    can_up, can_down = below[1], above[1]
    turn = [lax.rem(third + c, 4) * quarter for c in range(4)]

    def loads(block, tile, slot):
        z_ref, wo_ref, wi_ref = ((z_two, w2_out, w2_in), (z_one, w1_out, w1_in))[block]
        span = pl.ds(pl.multiple_of(tile * unit, 128), unit)
        return (
            pltpu.make_async_copy(z_ref.at[:, span], zbuf.at[slot], load_sem.at[slot, 0]),
            pltpu.make_async_copy(wo_ref.at[span, :], wo.at[slot], load_sem.at[slot, 1]),
            pltpu.make_async_copy(wi_ref.at[:, span], wi.at[slot], load_sem.at[slot, 2]),
        )

    dy_load = pltpu.make_async_copy(grad_out, dy, dy_sem)
    dy_load.start()
    for copy in loads(0, 0, 0):
        copy.start()
    pltpu.make_async_copy(x_two, xv, x_sem).start()

    barrier = pltpu.get_barrier_semaphore()
    for peer in (peer_core, peer_x, peer_y, peer_up, peer_down):
        pl.semaphore_signal(barrier, inc=1, device_id=peer, device_id_type=MESH)
    pl.semaphore_wait(barrier, 5)

    def remote(src, dst, i, k, peer):
        return pltpu.make_async_remote_copy(
            src_ref=src, dst_ref=dst, send_sem=send_sem.at[i, k], recv_sem=recv_sem.at[i, k],
            device_id=peer, device_id_type=MESH)

    def rows_loop(count, fn):
        block = math.gcd(count, 16)

        @pl.loop(0, count // block)
        def _(t):
            fn(pl.multiple_of(t * block, 8), block)

    def pair_copy(q, kind, i):
        slot = q % RING
        return remote(tiles.at[slot, kind, 1 - core], rec_d.at[slot, kind], i, 0, peer_core)

    def out_copies(i, kind, tile):
        block = tile // TILES
        out = outs[2 * block + kind]
        span = pl.ds(pl.multiple_of((tile - TILES * block + core) * unit, 128), unit)
        copies = []
        if kind == 0:
            pairs = [(acc.at[i], out.at[span, :])]
        else:
            pairs = [(acc.at[i, :, pl.ds(b * unit, unit)], out.at[pl.ds(b * unit, unit), span]) for b in range(width // unit)]
        for b, (src, dst) in enumerate(pairs):
            copies += [remote(src, dst, i, 13 + b, peer_core), pltpu.make_async_copy(src, dst, out_sem.at[i, b])]
        return copies

    class Chunk:
        def __init__(self, q, kind):
            self.q, self.kind, self.i = q, kind, 2 * q + kind
            colour = lax.rem(q + kind, 2)
            self.first_bit = x_bit + colour * (second - x_bit)
            self.last_bit = second + colour * (x_bit - second)
            self.first_peer = {'group': group + (1 - colour) * (2 - 4 * x_bit), 'second': second + colour * (1 - 2 * second)}
            self.last_peer = {'group': group + colour * (2 - 4 * x_bit), 'second': second + (1 - colour) * (1 - 2 * second)}
            self.kept = pl.multiple_of(self.first_bit * half, 8)
            self.other = pl.multiple_of(half - self.kept, 8)

        def span(self, row, count):
            return acc.at[self.i, pl.ds(pl.multiple_of(row, 8), count), :]

        def first(self):
            slot = 2 * (self.q % (PAIRS // 2)) + self.kind
            return remote(self.span(self.other, half), rec_first.at[slot], self.i, 1, self.first_peer)

        def up(self, place):
            rows = (3 - place) * quarter
            return remote(self.span(self.kept + (place + 1) * quarter, rows), rec_line.at[self.i, pl.ds(0, rows), :], self.i, 2, peer_up)

        def down(self, place):
            rows = place * quarter
            dst = rec_line.at[self.i, pl.ds((5 - place) * quarter, rows), :]
            return remote(self.span(self.kept, rows), dst, self.i, 3, peer_down)

        def mine(self):
            return self.kept + turn[0] + self.last_bit * piece

        def last(self):
            other = self.kept + turn[0] + (1 - self.last_bit) * piece
            return remote(self.span(other, piece), rec_last.at[self.i], self.i, 4, self.last_peer)

        def last_back(self):
            ref = self.span(self.mine(), piece)
            return remote(ref, ref, self.i, 5, self.last_peer)

        def spread_up(self, hop, arriving=0):
            ref = self.span(self.kept + turn[(5 - hop - arriving) % 4], quarter)
            return remote(ref, ref, self.i, 5 + hop, peer_up)

        def spread_down(self, hop, arriving=0):
            ref = self.span(self.kept + turn[(hop - 1 + arriving) % 4], quarter)
            return remote(ref, ref, self.i, 8 + hop, peer_down)

        def first_back(self):
            ref = self.span(self.kept, half)
            return remote(ref, ref, self.i, 12, self.first_peer)

    def signal(sem, peer):
        pl.semaphore_signal(sem, inc=1, device_id=peer, device_id_type=MESH)

    def add_rows(i, base, rec, rec_index, rec_base, count):
        def add(r, block):
            rows = pl.ds(pl.multiple_of(base + r, 8), block)
            acc[i, rows, :] += rec[rec_index, pl.ds(pl.multiple_of(rec_base + r, 8), block), :]

        rows_loop(count, add)

    def chunk_event(q, kind, stage):
        chunk = Chunk(q, kind)
        i, kept = chunk.i, chunk.kept
        if stage == 0:
            slot = q % RING
            got = pair_copy(q, kind, i)
            got.wait_recv()

            def first(base):
                def fn(r, block):
                    rows = pl.ds(pl.multiple_of(base + r, 8), block)
                    acc[i, rows, :] = tiles[slot, kind, core, rows, :].astype(jnp.float32) + rec_d[slot, kind, rows, :].astype(jnp.float32)
                return fn

            rows_loop(half, first(chunk.other))
            if q >= PAIRS // 2:
                pl.semaphore_wait(free_sem.at[i - PAIRS, 2], 1)
            chunk.first().start()
            rows_loop(half, first(kept))
            got.wait_send()
            if q + RING < PAIRS:
                signal(free_d.at[i], peer_core)
        elif stage == 1:
            got = chunk.first()
            got.wait_recv()
            add_rows(i, kept, rec_first, 2 * (q % (PAIRS // 2)) + kind, 0, half)

            @pl.when(at[0])
            def _():
                chunk.up(0).start()

            @pl.when(at[3])
            def _():
                chunk.down(3).start()

            if q < PAIRS // 2:
                signal(free_sem.at[i, 2], chunk.first_peer)
            got.wait_send()
            signal(free_sem.at[i, 0], chunk.first_peer)
        elif stage <= 4:
            hop = stage - 1

            @pl.when(at[hop])
            def _():
                chunk.up(hop - 1).wait_recv()
                add_rows(i, kept + hop * quarter, rec_line, i, 0, (4 - hop) * quarter)
                if hop < 3:
                    chunk.up(hop).start()

            @pl.when(at[3 - hop])
            def _():
                chunk.down(4 - hop).wait_recv()
                add_rows(i, kept, rec_line, i, (1 + hop) * quarter, (4 - hop) * quarter)
                if hop < 3:
                    chunk.down(3 - hop).start()

            if hop == 3:
                chunk.last().start()
        elif stage == 5:
            got = chunk.last()
            got.wait_recv()
            add_rows(i, chunk.mine(), rec_last, i, 0, piece)
            got.wait_send()
            signal(free_sem.at[i, 1], chunk.last_peer)
            pl.semaphore_wait(free_sem.at[i, 1], 1)
            chunk.last_back().start()
            for place in range(4):
                @pl.when(at[place])
                def _(place=place):
                    if place < 3:
                        chunk.up(place).wait_send()
                        signal(free_line.at[i, 0], peer_up)
                    if place > 0:
                        chunk.down(place).wait_send()
                        signal(free_line.at[i, 1], peer_down)
        elif stage == 6:
            chunk.last_back().wait_recv()

            @pl.when(can_up)
            def _():
                pl.semaphore_wait(free_line.at[i, 1], 1)
                chunk.spread_up(1).start()

            @pl.when(can_down)
            def _():
                pl.semaphore_wait(free_line.at[i, 0], 1)
                chunk.spread_down(1).start()
        elif stage <= 9:
            hop = stage - 6

            @pl.when(above[hop])
            def _():
                chunk.spread_up(hop, 1).wait_recv()
                if hop < 3:
                    @pl.when(can_up)
                    def _():
                        chunk.spread_up(hop + 1).start()

            @pl.when(below[hop])
            def _():
                chunk.spread_down(hop, 1).wait_recv()
                if hop < 3:
                    @pl.when(can_down)
                    def _():
                        chunk.spread_down(hop + 1).start()

            if hop == 3:
                pl.semaphore_wait(free_sem.at[i, 0], 1)
                chunk.first_back().start()
        else:
            chunk.first_back().wait_recv()

    def event(q, stage):
        @pl.loop(0, 2)
        def _(kind):
            chunk_event(q, kind, stage)

        if stage == 10:
            for kind in range(2):
                for copy in out_copies(2 * q + kind, kind, 2 * q):
                    copy.start()

    def run_events(step, point):
        span = 4
        for lo in range(0, 2 * TILES, span):
            if any(placed[k, point] for k in range(lo, lo + span)):
                @pl.when((step >= lo) & (step < lo + span))
                def _(lo=lo):
                    for k in range(lo, lo + span):
                        if placed[k, point]:
                            @pl.when(step == k)
                            def _(k=k):
                                for q, stage in placed[k, point]:
                                    event(q, stage)

    dy_load.wait()

    @pl.loop(0, tokens // rows_block)
    def _(r):
        rows = pl.ds(pl.multiple_of(r * rows_block, 16), rows_block)
        dx_acc[rows, :] = dy[rows, :].astype(jnp.float32)

    @pl.loop(0, 2 * TILES)
    def _(step):
        slot = step % 2
        for copy in loads(0, 0, slot):
            copy.wait()

        @pl.when(step < TILES - 1)
        def _():
            for copy in loads(0, step + 1, 1 - slot):
                copy.start()

        @pl.when((step >= TILES - 1) & (step < 2 * TILES - 1))
        def _():
            for copy in loads(1, step + 1 - TILES, 1 - slot):
                copy.start()

        def token_rows(r):
            rows = pl.ds(pl.multiple_of(r * rows_block, 128), rows_block)
            z_val = zbuf[slot, rows, :].astype(jnp.float32)
            cdf_val = 0.5 * (1.0 + lax.erf(z_val * INV_ROOT_TWO))
            ht[:, rows] = (z_val * cdf_val).astype(jnp.bfloat16).T
            slope = cdf_val + z_val * jnp.exp(-0.5 * z_val * z_val) * INV_ROOT_TWO_PI
            grad_hidden = lax.dot_general(dy[rows, :], wo[slot], CONTRACT_COLS, preferred_element_type=jnp.float32)
            grad_pre = (grad_hidden * slope).astype(jnp.bfloat16)
            dzt[:, rows] = grad_pre.T
            dx_acc[rows, :] += lax.dot_general(grad_pre, wi[slot], CONTRACT_COLS, preferred_element_type=jnp.float32)

        split = max(1, tokens // rows_block // 2)
        pl.loop(0, split)(token_rows)
        run_events(step, 0)
        pl.loop(split, tokens // rows_block)(token_rows)
        run_events(step, 1)

        pair = (step // 2) % RING
        tiles[pair, 0, slot] = lax.dot_general(ht[...], dy[...], CONTRACT_PLAIN, preferred_element_type=jnp.float32).astype(jnp.bfloat16)
        run_events(step, 2)

        @pl.when((step == 0) | (step == TILES))
        def _():
            pltpu.make_async_copy(x_two, xv, x_sem).wait()

        for b in range(width // unit):
            cols = pl.ds(b * unit, unit)
            tile = lax.dot_general(dzt[...], xv[:, cols], CONTRACT_PLAIN, preferred_element_type=jnp.float32)
            tiles[pair, 1, slot, :, cols] = tile.T.astype(jnp.bfloat16)

        @pl.when((step == TILES - 1) | (step == 2 * TILES - 1))
        def _():
            @pl.loop(0, tokens // rows_block)
            def _(r):
                rows = pl.ds(pl.multiple_of(r * rows_block, 16), rows_block)
                grad_x = dx_acc[rows, :].astype(jnp.bfloat16)
                dy[rows, :] = grad_x
                dx_acc[rows, :] = grad_x.astype(jnp.float32)

        @pl.when(step == TILES - 1)
        def _():
            pltpu.make_async_copy(x_one, xv, x_sem).start()

        @pl.when(slot == 1)
        def _():
            q = step // 2
            for kind in range(2):
                i = 2 * q + kind

                @pl.when(q >= RING)
                def _():
                    pl.semaphore_wait(free_d.at[i - 2 * RING], 1)

                pair_copy(q, kind, i).start()

        run_events(step, 3)

    dx_store = pltpu.make_async_copy(dy, dx_out, dx_sem)
    dx_store.start()
    for q, stage in tail:
        event(q, stage)
    dx_store.wait()

    @pl.loop(0, PAIRS)
    def _(q):
        for kind in range(2):
            chunk = Chunk(q, kind)
            chunk.last_back().wait_send()
            for hop in range(1, 4):
                @pl.when(above[hop - 1] & can_up)
                def _(chunk=chunk, hop=hop):
                    chunk.spread_up(hop).wait_send()

                @pl.when(below[hop - 1] & can_down)
                def _(chunk=chunk, hop=hop):
                    chunk.spread_down(hop).wait_send()
            chunk.first_back().wait_send()

    for q in range(PAIRS):
        for kind in range(2):
            for copy in out_copies(2 * q + kind, kind, 2 * q):
                copy.wait()


def backward_and_reduce(x_one, z_one, x_two, z_two, grad_out, w1_in, w1_out, w2_in, w2_out):
    tokens, width = x_one.shape
    hidden = z_one.shape[1]
    unit = hidden // TILES
    any_spec = pl.BlockSpec(memory_space=pl.ANY)
    bf16, f32 = jnp.bfloat16, jnp.float32
    return pl.pallas_call(
        step_kernel,
        name='backward_and_reduce',
        out_shape=[jax.ShapeDtypeStruct((hidden, width), f32), jax.ShapeDtypeStruct((width, hidden), f32)] * 2 + [jax.ShapeDtypeStruct((tokens, width), bf16)],
        in_specs=[any_spec] * 9,
        out_specs=[any_spec] * 5,
        scratch_shapes=[
            pltpu.VMEM((CHUNKS, unit, width), f32),
            pltpu.VMEM((PAIRS, unit // 2, width), f32),
            pltpu.VMEM((CHUNKS, 5 * unit // 8, width), f32),
            pltpu.VMEM((CHUNKS, unit // 16, width), f32),
            pltpu.VMEM((RING, 2, unit, width), bf16),
            pltpu.VMEM((RING, 2, 2, unit, width), bf16),
            pltpu.VMEM((tokens, width), bf16),
            pltpu.VMEM((tokens, width), bf16),
            pltpu.VMEM((tokens, width), f32),
            pltpu.VMEM((2, tokens, unit), bf16),
            pltpu.VMEM((2, unit, width), bf16),
            pltpu.VMEM((2, width, unit), bf16),
            pltpu.VMEM((unit, tokens), bf16),
            pltpu.VMEM((unit, tokens), bf16),
            pltpu.SemaphoreType.DMA((CHUNKS, 13 + width // unit)),
            pltpu.SemaphoreType.DMA((CHUNKS, 13 + width // unit)),
            pltpu.SemaphoreType.DMA((CHUNKS, width // unit)),
            pltpu.SemaphoreType.DMA((2, 3)),
            pltpu.SemaphoreType.DMA,
            pltpu.SemaphoreType.DMA,
            pltpu.SemaphoreType.DMA,
            pltpu.SemaphoreType.REGULAR((CHUNKS, 3)),
            pltpu.SemaphoreType.REGULAR((CHUNKS, 2)),
            pltpu.SemaphoreType.REGULAR((CHUNKS,)),
        ],
        compiler_params=pltpu.CompilerParams(
            collective_id=0, has_side_effects=True, vmem_limit_bytes=67043328),
    )(x_two, z_two, grad_out, w2_in, w2_out, x_one, z_one, w1_in, w1_out)


def solution(mesh):
    def device_step(*args):
        return tuple(backward_and_reduce(*args))

    row_spec = P(AXES, None)
    repl_spec = P()
    return jax.shard_map(
        device_step,
        mesh=mesh,
        in_specs=(row_spec, row_spec, row_spec, row_spec, row_spec, repl_spec, repl_spec, repl_spec, repl_spec),
        out_specs=(repl_spec, repl_spec, repl_spec, repl_spec, row_spec),
        check_vma=False,
    )
```

```python
import functools
import math
import jax
import jax.numpy as jnp
from jax import lax
from jax.experimental import pallas as pl
from jax.experimental.pallas import tpu as pltpu
from jax.sharding import PartitionSpec as P

AXES = ('third', 'second', 'group')
INV_ROOT_TWO = math.sqrt(0.5)
INV_ROOT_TWO_PI = 1.0 / math.sqrt(2.0 * math.pi)
CONTRACT_COLS = (((1,), (1,)), ((), ()))
CONTRACT_PLAIN = (((1,), (0,)), ((), ()))
MESH = pl.DeviceIdType.MESH
TILES = 12
PAIRS = TILES
CHUNKS = 2 * PAIRS
RING = 3
POINTS = 4
ORDER = (
    -1, -1, -1, -1, -1, -1, -1, -1, -1, 0, -1, -1, -1, -1, -1, -1, 1, -1, -1, 11, -1, -1, -1, -1,
    -1, 2, 12, -1, -1, -1, 22, -1, -1, 3, -1, -1, -1, 4, 13, 23, -1, 5, -1, -1, 33, 6, -1, -1,
    14, -1, -1, 24, -1, 34, 15, -1, 7, -1, -1, 16, 44, 25, 17, -1, -1, -1, 35, 8, 26, -1, 45, 18,
    27, -1, 9, -1, 28, -1, -1, 36, 55, 19, -1, 46, -1, -1, -1, 29, 37, 20, -1, 56, 38, 47, -1, -1,
    -1, 30, 66, -1, 39, -1, 48, -1, 31, 57, -1, -1, 67, 40, -1, -1, 10, 49, 58, 21, 77, -1, 50, -1,
    41, -1, 68, 59, -1, -1, 51, 78, 60, 42, -1, -1, -1, 32, 69, -1, 88, 52, 61, -1, -1, 79, -1, -1,
    70, 53, -1, 62, 89, -1, -1, 80, 71, -1, 99, 63, -1, 72, -1, -1, 90, 81, -1, 64, -1, 100, 73, -1,
    -1, 82, 91, 110, -1, 83, -1, 92, -1, 74, 101, -1, -1, 84, 111, 93, 75, -1, 54, 94, -1, -1, 85, 102,
    121, 112, 95, 103, 113, 122, 104, 114, 96, 105, 115, 65, 86, 116, 76, 123, 97, 106, 117, 124, 125, 107, 126, 108,
    127, 87, 118, 128, 119, 129, 130, 98, 43, 109, 120, 131,
)


def event_plan():
    placed = {(step, point): [] for step in range(2 * TILES) for point in range(POINTS)}
    quarters, tail = 0, []
    for entry in ORDER:
        if entry < 0:
            quarters += 1
        elif quarters < 2 * TILES * POINTS:
            placed[(quarters - 1) // POINTS, (quarters - 1) % POINTS].append(divmod(entry, 11))
        else:
            tail.append(divmod(entry, 11))
    return placed, tail


def step_kernel(*refs):
    x_two, z_two, grad_out, w2_in, w2_out, x_one, z_one, w1_in, w1_out = refs[:9]
    outs, dx_out = refs[9:13], refs[13]
    (acc, rec_first, rec_line, rec_last, rec_d, tiles, dy, xv, dx_acc, zbuf, wo, wi, ht, dzt,
     send_sem, recv_sem, out_sem, load_sem, dy_sem, x_sem, dx_sem, free_sem, free_line, free_d) = refs[14:]
    unit, width = acc.shape[1], acc.shape[2]
    tokens = dy.shape[0]
    rows_block = min(256, tokens)
    placed, tail = event_plan()
    group, second, third = lax.axis_index('group'), lax.axis_index('second'), lax.axis_index('third')
    core, x_bit = lax.rem(group, 2), group // 2
    half, quarter, piece = unit // 2, unit // 8, unit // 16
    peer_core = {'group': group + 1 - 2 * core}
    peer_x = {'group': group + 2 - 4 * x_bit}
    peer_y = {'second': 1 - second}
    peer_up, peer_down = {'third': lax.rem(third + 1, 4)}, {'third': lax.rem(third + 3, 4)}
    at = [third == place for place in range(4)]
    above, below = [third >= hop for hop in range(4)], [third <= 3 - hop for hop in range(4)]
    can_up, can_down = below[1], above[1]
    turn = [lax.rem(third + c, 4) * quarter for c in range(4)]

    def loads(block, tile, slot):
        z_ref, wo_ref, wi_ref = ((z_two, w2_out, w2_in), (z_one, w1_out, w1_in))[block]
        span = pl.ds(pl.multiple_of(tile * unit, 128), unit)
        return (
            pltpu.make_async_copy(z_ref.at[:, span], zbuf.at[slot], load_sem.at[slot, 0]),
            pltpu.make_async_copy(wo_ref.at[span, :], wo.at[slot], load_sem.at[slot, 1]),
            pltpu.make_async_copy(wi_ref.at[:, span], wi.at[slot], load_sem.at[slot, 2]),
        )

    dy_load = pltpu.make_async_copy(grad_out, dy, dy_sem)
    dy_load.start()
    for copy in loads(0, 0, 0):
        copy.start()
    pltpu.make_async_copy(x_two, xv, x_sem).start()

    barrier = pltpu.get_barrier_semaphore()
    for peer in (peer_core, peer_x, peer_y, peer_up, peer_down):
        pl.semaphore_signal(barrier, inc=1, device_id=peer, device_id_type=MESH)
    pl.semaphore_wait(barrier, 5)

    def remote(src, dst, i, k, peer):
        return pltpu.make_async_remote_copy(
            src_ref=src, dst_ref=dst, send_sem=send_sem.at[i, k], recv_sem=recv_sem.at[i, k],
            device_id=peer, device_id_type=MESH)

    def rows_loop(count, fn):
        block = math.gcd(count, 32)

        @pl.loop(0, count // block)
        def _(t):
            fn(pl.multiple_of(t * block, 8), block)

    def pair_copy(q, kind, i):
        slot = q % RING
        return remote(tiles.at[slot, kind, 1 - core], rec_d.at[slot, kind], i, 0, peer_core)

    def out_copies(i, kind, tile):
        block = tile // TILES
        out = outs[2 * block + kind]
        span = pl.ds(pl.multiple_of((tile - TILES * block + core) * unit, 128), unit)
        copies = []
        if kind == 0:
            pairs = [(acc.at[i], out.at[span, :])]
        else:
            pairs = [(acc.at[i, :, pl.ds(b * unit, unit)], out.at[pl.ds(b * unit, unit), span]) for b in range(width // unit)]
        for b, (src, dst) in enumerate(pairs):
            copies += [remote(src, dst, i, 13 + b, peer_core), pltpu.make_async_copy(src, dst, out_sem.at[i, b])]
        return copies

    class Chunk:
        def __init__(self, q, kind):
            self.q, self.kind, self.i = q, kind, 2 * q + kind
            colour = lax.rem(q + kind, 2)
            self.first_bit = x_bit + colour * (second - x_bit)
            self.last_bit = second + colour * (x_bit - second)
            self.first_peer = {'group': group + (1 - colour) * (2 - 4 * x_bit), 'second': second + colour * (1 - 2 * second)}
            self.last_peer = {'group': group + colour * (2 - 4 * x_bit), 'second': second + (1 - colour) * (1 - 2 * second)}
            self.kept = pl.multiple_of(self.first_bit * half, 8)
            self.other = pl.multiple_of(half - self.kept, 8)

        def span(self, row, count):
            return acc.at[self.i, pl.ds(pl.multiple_of(row, 8), count), :]

        def first(self):
            slot = 2 * (self.q % (PAIRS // 2)) + self.kind
            return remote(self.span(self.other, half), rec_first.at[slot], self.i, 1, self.first_peer)

        def up(self, place):
            rows = (3 - place) * quarter
            return remote(self.span(self.kept + (place + 1) * quarter, rows), rec_line.at[self.i, pl.ds(0, rows), :], self.i, 2, peer_up)

        def down(self, place):
            rows = place * quarter
            dst = rec_line.at[self.i, pl.ds((5 - place) * quarter, rows), :]
            return remote(self.span(self.kept, rows), dst, self.i, 3, peer_down)

        def mine(self):
            return self.kept + turn[0] + self.last_bit * piece

        def last(self):
            other = self.kept + turn[0] + (1 - self.last_bit) * piece
            return remote(self.span(other, piece), rec_last.at[self.i], self.i, 4, self.last_peer)

        def last_back(self):
            ref = self.span(self.mine(), piece)
            return remote(ref, ref, self.i, 5, self.last_peer)

        def spread_up(self, hop, arriving=0):
            ref = self.span(self.kept + turn[(5 - hop - arriving) % 4], quarter)
            return remote(ref, ref, self.i, 5 + hop, peer_up)

        def spread_down(self, hop, arriving=0):
            ref = self.span(self.kept + turn[(hop - 1 + arriving) % 4], quarter)
            return remote(ref, ref, self.i, 8 + hop, peer_down)

        def first_back(self):
            ref = self.span(self.kept, half)
            return remote(ref, ref, self.i, 12, self.first_peer)

    def signal(sem, peer):
        pl.semaphore_signal(sem, inc=1, device_id=peer, device_id_type=MESH)

    def add_rows(i, base, rec, rec_index, rec_base, count):
        def add(r, block):
            rows = pl.ds(pl.multiple_of(base + r, 8), block)
            acc[i, rows, :] += rec[rec_index, pl.ds(pl.multiple_of(rec_base + r, 8), block), :]

        rows_loop(count, add)

    def chunk_event(q, kind, stage):
        chunk = Chunk(q, kind)
        i, kept = chunk.i, chunk.kept
        if stage == 0:
            slot = q % RING
            got = pair_copy(q, kind, i)
            got.wait_recv()

            def first(base):
                def fn(r, block):
                    rows = pl.ds(pl.multiple_of(base + r, 8), block)
                    acc[i, rows, :] = tiles[slot, kind, core, rows, :].astype(jnp.float32) + rec_d[slot, kind, rows, :].astype(jnp.float32)
                return fn

            rows_loop(half, first(chunk.other))
            if q >= PAIRS // 2:
                pl.semaphore_wait(free_sem.at[i - PAIRS, 2], 1)
            chunk.first().start()
            rows_loop(half, first(kept))
            got.wait_send()
            if q + RING < PAIRS:
                signal(free_d.at[i], peer_core)
        elif stage == 1:
            got = chunk.first()
            got.wait_recv()
            add_rows(i, kept, rec_first, 2 * (q % (PAIRS // 2)) + kind, 0, half)

            @pl.when(at[0])
            def _():
                chunk.up(0).start()

            @pl.when(at[3])
            def _():
                chunk.down(3).start()

            if q < PAIRS // 2:
                signal(free_sem.at[i, 2], chunk.first_peer)
            got.wait_send()
            signal(free_sem.at[i, 0], chunk.first_peer)
        elif stage <= 4:
            hop = stage - 1

            @pl.when(at[hop])
            def _():
                chunk.up(hop - 1).wait_recv()
                add_rows(i, kept + hop * quarter, rec_line, i, 0, (4 - hop) * quarter)
                if hop < 3:
                    chunk.up(hop).start()

            @pl.when(at[3 - hop])
            def _():
                chunk.down(4 - hop).wait_recv()
                add_rows(i, kept, rec_line, i, (1 + hop) * quarter, (4 - hop) * quarter)
                if hop < 3:
                    chunk.down(3 - hop).start()

            if hop == 3:
                chunk.last().start()
        elif stage == 5:
            got = chunk.last()
            got.wait_recv()
            add_rows(i, chunk.mine(), rec_last, i, 0, piece)
            got.wait_send()
            signal(free_sem.at[i, 1], chunk.last_peer)
            pl.semaphore_wait(free_sem.at[i, 1], 1)
            chunk.last_back().start()
            for place in range(4):
                @pl.when(at[place])
                def _(place=place):
                    if place < 3:
                        chunk.up(place).wait_send()
                        signal(free_line.at[i, 0], peer_up)
                    if place > 0:
                        chunk.down(place).wait_send()
                        signal(free_line.at[i, 1], peer_down)
        elif stage == 6:
            chunk.last_back().wait_recv()

            @pl.when(can_up)
            def _():
                pl.semaphore_wait(free_line.at[i, 1], 1)
                chunk.spread_up(1).start()

            @pl.when(can_down)
            def _():
                pl.semaphore_wait(free_line.at[i, 0], 1)
                chunk.spread_down(1).start()
        elif stage <= 9:
            hop = stage - 6

            @pl.when(above[hop])
            def _():
                chunk.spread_up(hop, 1).wait_recv()
                if hop < 3:
                    @pl.when(can_up)
                    def _():
                        chunk.spread_up(hop + 1).start()

            @pl.when(below[hop])
            def _():
                chunk.spread_down(hop, 1).wait_recv()
                if hop < 3:
                    @pl.when(can_down)
                    def _():
                        chunk.spread_down(hop + 1).start()

            if hop == 3:
                pl.semaphore_wait(free_sem.at[i, 0], 1)
                chunk.first_back().start()
        else:
            chunk.first_back().wait_recv()

    def event(q, stage):
        @pl.loop(0, 2)
        def _(kind):
            chunk_event(q, kind, stage)

        if stage == 10:
            for kind in range(2):
                for copy in out_copies(2 * q + kind, kind, 2 * q):
                    copy.start()

    def run_events(step, point):
        span = 4
        for lo in range(0, 2 * TILES, span):
            if any(placed[k, point] for k in range(lo, lo + span)):
                @pl.when((step >= lo) & (step < lo + span))
                def _(lo=lo):
                    for k in range(lo, lo + span):
                        if placed[k, point]:
                            @pl.when(step == k)
                            def _(k=k):
                                for q, stage in placed[k, point]:
                                    event(q, stage)

    dy_load.wait()

    @pl.loop(0, tokens // rows_block)
    def _(r):
        rows = pl.ds(pl.multiple_of(r * rows_block, 16), rows_block)
        dx_acc[rows, :] = dy[rows, :].astype(jnp.float32)

    @pl.loop(0, 2 * TILES)
    def _(step):
        slot = step % 2
        for copy in loads(0, 0, slot):
            copy.wait()

        @pl.when(step < TILES - 1)
        def _():
            for copy in loads(0, step + 1, 1 - slot):
                copy.start()

        @pl.when((step >= TILES - 1) & (step < 2 * TILES - 1))
        def _():
            for copy in loads(1, step + 1 - TILES, 1 - slot):
                copy.start()

        def token_rows(r):
            rows = pl.ds(pl.multiple_of(r * rows_block, 128), rows_block)
            z_val = zbuf[slot, rows, :].astype(jnp.float32)
            cdf_val = 0.5 * (1.0 + lax.erf(z_val * INV_ROOT_TWO))
            ht[:, rows] = (z_val * cdf_val).astype(jnp.bfloat16).T
            slope = cdf_val + z_val * jnp.exp(-0.5 * z_val * z_val) * INV_ROOT_TWO_PI
            grad_hidden = lax.dot_general(dy[rows, :], wo[slot], CONTRACT_COLS, preferred_element_type=jnp.float32)
            grad_pre = (grad_hidden * slope).astype(jnp.bfloat16)
            dzt[:, rows] = grad_pre.T
            dx_acc[rows, :] += lax.dot_general(grad_pre, wi[slot], CONTRACT_COLS, preferred_element_type=jnp.float32)

        split = max(1, tokens // rows_block // 2)
        pl.loop(0, split)(token_rows)
        run_events(step, 0)
        pl.loop(split, tokens // rows_block)(token_rows)
        run_events(step, 1)

        pair = (step // 2) % RING
        tiles[pair, 0, slot] = lax.dot_general(ht[...], dy[...], CONTRACT_PLAIN, preferred_element_type=jnp.float32).astype(jnp.bfloat16)
        run_events(step, 2)

        @pl.when((step == 0) | (step == TILES))
        def _():
            pltpu.make_async_copy(x_two, xv, x_sem).wait()

        for b in range(width // unit):
            cols = pl.ds(b * unit, unit)
            tile = lax.dot_general(dzt[...], xv[:, cols], CONTRACT_PLAIN, preferred_element_type=jnp.float32)
            tiles[pair, 1, slot, :, cols] = tile.T.astype(jnp.bfloat16)

        @pl.when((step == TILES - 1) | (step == 2 * TILES - 1))
        def _():
            @pl.loop(0, tokens // rows_block)
            def _(r):
                rows = pl.ds(pl.multiple_of(r * rows_block, 16), rows_block)
                grad_x = dx_acc[rows, :].astype(jnp.bfloat16)
                dy[rows, :] = grad_x
                dx_acc[rows, :] = grad_x.astype(jnp.float32)

        @pl.when(step == TILES - 1)
        def _():
            pltpu.make_async_copy(x_one, xv, x_sem).start()

        @pl.when(slot == 1)
        def _():
            q = step // 2
            for kind in range(2):
                i = 2 * q + kind

                @pl.when(q >= RING)
                def _():
                    pl.semaphore_wait(free_d.at[i - 2 * RING], 1)

                pair_copy(q, kind, i).start()

        run_events(step, 3)

    dx_store = pltpu.make_async_copy(dy, dx_out, dx_sem)
    dx_store.start()
    for q, stage in tail:
        event(q, stage)
    dx_store.wait()

    @pl.loop(0, PAIRS)
    def _(q):
        for kind in range(2):
            chunk = Chunk(q, kind)
            chunk.last_back().wait_send()
            for hop in range(1, 4):
                @pl.when(above[hop - 1] & can_up)
                def _(chunk=chunk, hop=hop):
                    chunk.spread_up(hop).wait_send()

                @pl.when(below[hop - 1] & can_down)
                def _(chunk=chunk, hop=hop):
                    chunk.spread_down(hop).wait_send()
            chunk.first_back().wait_send()

    for q in range(PAIRS):
        for kind in range(2):
            for copy in out_copies(2 * q + kind, kind, 2 * q):
                copy.wait()


def backward_and_reduce(x_one, z_one, x_two, z_two, grad_out, w1_in, w1_out, w2_in, w2_out):
    tokens, width = x_one.shape
    hidden = z_one.shape[1]
    unit = hidden // TILES
    any_spec = pl.BlockSpec(memory_space=pl.ANY)
    bf16, f32 = jnp.bfloat16, jnp.float32
    return pl.pallas_call(
        step_kernel,
        name='backward_and_reduce',
        out_shape=[jax.ShapeDtypeStruct((hidden, width), f32), jax.ShapeDtypeStruct((width, hidden), f32)] * 2 + [jax.ShapeDtypeStruct((tokens, width), bf16)],
        in_specs=[any_spec] * 9,
        out_specs=[any_spec] * 5,
        scratch_shapes=[
            pltpu.VMEM((CHUNKS, unit, width), f32),
            pltpu.VMEM((PAIRS, unit // 2, width), f32),
            pltpu.VMEM((CHUNKS, 5 * unit // 8, width), f32),
            pltpu.VMEM((CHUNKS, unit // 16, width), f32),
            pltpu.VMEM((RING, 2, unit, width), bf16),
            pltpu.VMEM((RING, 2, 2, unit, width), bf16),
            pltpu.VMEM((tokens, width), bf16),
            pltpu.VMEM((tokens, width), bf16),
            pltpu.VMEM((tokens, width), f32),
            pltpu.VMEM((2, tokens, unit), bf16),
            pltpu.VMEM((2, unit, width), bf16),
            pltpu.VMEM((2, width, unit), bf16),
            pltpu.VMEM((unit, tokens), bf16),
            pltpu.VMEM((unit, tokens), bf16),
            pltpu.SemaphoreType.DMA((CHUNKS, 13 + width // unit)),
            pltpu.SemaphoreType.DMA((CHUNKS, 13 + width // unit)),
            pltpu.SemaphoreType.DMA((CHUNKS, width // unit)),
            pltpu.SemaphoreType.DMA((2, 3)),
            pltpu.SemaphoreType.DMA,
            pltpu.SemaphoreType.DMA,
            pltpu.SemaphoreType.DMA,
            pltpu.SemaphoreType.REGULAR((CHUNKS, 3)),
            pltpu.SemaphoreType.REGULAR((CHUNKS, 2)),
            pltpu.SemaphoreType.REGULAR((CHUNKS,)),
        ],
        compiler_params=pltpu.CompilerParams(
            collective_id=0, has_side_effects=True, vmem_limit_bytes=67043328),
    )(x_two, z_two, grad_out, w2_in, w2_out, x_one, z_one, w1_in, w1_out)


def solution(mesh):
    def device_step(*args):
        return tuple(backward_and_reduce(*args))

    row_spec = P(AXES, None)
    repl_spec = P()
    return jax.shard_map(
        device_step,
        mesh=mesh,
        in_specs=(row_spec, row_spec, row_spec, row_spec, row_spec, repl_spec, repl_spec, repl_spec, repl_spec),
        out_specs=(repl_spec, repl_spec, repl_spec, repl_spec, row_spec),
        check_vma=False,
    )
```
